32 devices in a mesh: dom: 32 (over z, y, x, core).
Axes of the slice: x: 2, y: 2, z: 4, core: 2. Of those that a mesh axis runs over, the one named last changes fastest.
Arguments:
- features: bfloat16 [32768, 256], P('dom'), may hold values from -6 to 6
- edge_source: int32 [32, 128, 128], P('dom'), may hold values from 0 to 2047, as said below
- edge_relation: int32 [32, 128, 128], P('dom'), may hold values from 0 to 7
- edge_target: int32 [32, 128, 128], P('dom'), may hold values from 0 to 1023, as said below
- block_count: int32 [32], P('dom'), may hold values from 1 to 128, as said below
- send_list: int32 [32, 32, 32], P('dom'), may hold values from 0 to 1023
- bases_first: bfloat16 [30, 256, 256], P(None, 'dom'), may hold values from -0.375 to 0.375
- self_first: bfloat16 [256, 256], P('dom'), may hold values from -0.375 to 0.375
- coef_first: float32 [8, 30], replicated, may hold values from -1 to 1
- bias_first: float32 [256], replicated, may hold values from -3 to 3
- bases_second: bfloat16 [30, 256, 256], P(None, 'dom'), may hold values from -0.375 to 0.375
- self_second: bfloat16 [256, 256], P('dom'), may hold values from -0.375 to 0.375
- coef_second: float32 [8, 30], replicated, may hold values from -1 to 1
- bias_second: float32 [256], replicated, may hold values from -3 to 3
Outputs:
- embedded: bfloat16 [32768, 256], P('dom')
The draws below stay inside these ranges and needn't reach their ends.
Inputs may be any that keep to these rules, and one draw needn't show every extreme that they name: `edge_source`: an entry below 1024 names a row of the edge's own partition; an entry 1024 + p * 32 + s names the row that partition p sends to the edge's partition in slot s, and p is never the edge's own partition. `edge_target`: non-decreasing within each block; all targets of one block lie in one aligned window of 16 rows, from 16 * k to 16 * k + 15 for some k. `block_count`: blocks at and beyond it are ignored; some partition uses all 128.
All inputs are finite; a program needn't handle non-finite values.
Results may differ from the reference program's by a relative error of at most 0.0064.
Values may be sent and summed in bfloat16 or wider, within the bound.
A program may use at most 128 MiB of HBM per device.

```python
import jax
import jax.numpy as jnp
from jax import lax

D = 256
REL = 8
BASES = 30
NODE_DEV = 1024
SLOT = 32
BLOCKS = 128
EBLK = 128
WIN = 16
NODES = 32768
N_DOM = 32


def draw_edge_source(key, part):
    key_used, key_local, key_offset, key_slot, key_remote = jax.random.split(key, 5)
    shape = (N_DOM, BLOCKS, EBLK)
    sent_counts = jax.random.randint(key_used, (N_DOM, N_DOM), SLOT // 4, SLOT + 1)
    local_rows = jax.random.randint(key_local, shape, 0, NODE_DEV)
    offset = jax.random.randint(key_offset, shape, 1, N_DOM)
    target_part = jnp.arange(N_DOM, dtype=jnp.int32)[:, None, None]
    owner = (target_part + offset) % N_DOM
    limit = sent_counts[owner, target_part]
    slot_index = jax.random.randint(key_slot, shape, 0, 1 << 20) % limit
    remote = jax.random.randint(key_remote, shape, 0, 2) == 1
    return jnp.where(remote, NODE_DEV + owner * SLOT + slot_index, local_rows).astype(jnp.int32)


def draw_edge_target(key, part):
    key_window, key_offset = jax.random.split(key)
    windows = jnp.sort(jax.random.randint(key_window, (N_DOM, BLOCKS), 0, NODE_DEV // WIN), axis=1)
    offsets = jnp.sort(jax.random.randint(key_offset, (N_DOM, BLOCKS, EBLK), 0, WIN), axis=2)
    return (windows[:, :, None] * WIN + offsets).astype(jnp.int32)


def draw_block_count(key, part):
    key_counts, key_top = jax.random.split(key)
    counts = jax.random.randint(key_counts, (N_DOM,), max(BLOCKS // 2, 1), BLOCKS + 1)
    busiest = jax.random.randint(key_top, (), 0, N_DOM)
    return counts.at[busiest].set(BLOCKS).astype(jnp.int32)


def place_ends(entries, own_key, least, largest):
    spot = [jax.random.randint(jax.random.fold_in(own_key, axis), (), 0, length) for axis, length in enumerate(entries.shape)]
    main_axis = entries.shape.index(max(entries.shape))
    next_to = spot[:main_axis] + [(spot[main_axis] + 1) % entries.shape[main_axis]] + spot[main_axis + 1:]
    return entries.at[tuple(spot)].set(least).at[tuple(next_to)].set(largest)


def steps_of(own_key, shape, cuts, least, top_value):
    loudness = 1.0
    for dim, blocks in cuts:
        heights = jax.random.uniform(jax.random.fold_in(jax.random.fold_in(own_key, 6), dim), (blocks,), jnp.float32, least / len(cuts), top_value / len(cuts))
        loudness = loudness * jnp.repeat(jnp.exp(heights), shape[dim] // blocks).reshape((-1,) + (1,) * (len(shape) - 1 - dim))
    return loudness


def scatter_about(rng, dims, deviation, most, pieces=(), kind=jnp.bfloat16):
    drawn = deviation * jax.random.normal(rng, dims, jnp.float32)
    if pieces:
        drawn = drawn * steps_of(rng, dims, pieces, -0.22, 0.18)
    return jnp.clip(drawn, -most, most).astype(kind)


def setup_inputs(seed: int = 0) -> dict:
    streams_of = jax.random.split(jax.random.key(seed), 15)
    return {
        "features": scatter_about(streams_of[0], (NODES, D), 1.0, 6.0, ((0, 32),)),
        "edge_source": draw_edge_source(jax.random.fold_in(streams_of[14], 71), 0),
        "edge_relation": place_ends(jax.random.randint(streams_of[2], (N_DOM, BLOCKS, EBLK), 0, REL), jax.random.fold_in(streams_of[2], 1), 0, REL - 1).astype(jnp.int32),
        "edge_target": draw_edge_target(jax.random.fold_in(streams_of[14], 71), 0),
        "block_count": draw_block_count(jax.random.fold_in(streams_of[14], 71), 0),
        "send_list": place_ends(jax.random.randint(streams_of[5], (N_DOM, N_DOM, SLOT), 0, NODE_DEV), jax.random.fold_in(streams_of[5], 1), 0, NODE_DEV - 1).astype(jnp.int32),
        "bases_first": scatter_about(streams_of[6], (BASES, D, D), D ** -0.5, 0.375, ((1, 32),)),
        "self_first": scatter_about(streams_of[7], (D, D), D ** -0.5, 0.375, ((0, 32),)),
        "coef_first": scatter_about(streams_of[8], (REL, BASES), BASES ** -0.5, 1.0, (), jnp.float32),
        "bias_first": scatter_about(streams_of[9], (D,), 0.5, 3.0, (), jnp.float32),
        "bases_second": scatter_about(streams_of[10], (BASES, D, D), D ** -0.5, 0.375, ((1, 32),)),
        "self_second": scatter_about(streams_of[11], (D, D), D ** -0.5, 0.375, ((0, 32),)),
        "coef_second": scatter_about(streams_of[12], (REL, BASES), BASES ** -0.5, 1.0, (), jnp.float32),
        "bias_second": scatter_about(streams_of[13], (D,), 0.5, 3.0, (), jnp.float32),
    }


def compose_weights(coef, bases):
    mixed = jnp.einsum("rb,bij->rij", coef, bases.astype(jnp.float32), precision=lax.Precision.HIGHEST)
    return mixed.astype(jnp.bfloat16)


def relational_layer(inputs_now, edge_source, edge_relation, edge_target, block_count, send_list, mixed, self_weight, bias):
    owners = jnp.arange(N_DOM, dtype=jnp.int32)

    def one_part(part_index):
        received = inputs_now[owners[:, None], send_list[:, part_index, :]].reshape(-1, D)
        row_table = jnp.concatenate([inputs_now[part_index], received], axis=0)
        sources = edge_source[part_index].reshape(-1)
        relation_ids = edge_relation[part_index].reshape(-1)
        targets = edge_target[part_index].reshape(-1)
        block_ids = lax.broadcasted_iota(jnp.int32, (BLOCKS, EBLK), 0).reshape(-1)
        in_use = block_ids < block_count[part_index]
        messages = row_table[sources].astype(jnp.float32)
        segment = jnp.where(in_use, targets * REL + relation_ids, NODE_DEV * REL)
        degree = jax.ops.segment_sum(jnp.ones(segment.shape, jnp.float32), segment, NODE_DEV * REL + 1)[:NODE_DEV * REL]
        pooled = jax.ops.segment_sum(messages, segment, NODE_DEV * REL + 1)[:NODE_DEV * REL]
        averaged = (pooled / jnp.maximum(degree, 1.0)[:, None]).astype(jnp.bfloat16).reshape(NODE_DEV, REL, D)
        summed_all = jnp.dot(inputs_now[part_index], self_weight, preferred_element_type=jnp.float32) + bias
        for relation in range(REL):
            summed_all = summed_all + jnp.dot(averaged[:, relation, :], mixed[relation], preferred_element_type=jnp.float32)
        return summed_all

    return lax.map(one_part, owners)


def reference(features, edge_source, edge_relation, edge_target, block_count, send_list, bases_first, self_first, coef_first, bias_first, bases_second, self_second, coef_second, bias_second):
    inputs_now = features.reshape(N_DOM, NODE_DEV, D)
    mixed_first = compose_weights(coef_first, bases_first)
    first = relational_layer(inputs_now, edge_source, edge_relation, edge_target, block_count, send_list, mixed_first, self_first, bias_first)
    hidden = jnp.maximum(first, 0.0).astype(jnp.bfloat16)
    mixed_second = compose_weights(coef_second, bases_second)
    second = relational_layer(hidden, edge_source, edge_relation, edge_target, block_count, send_list, mixed_second, self_second, bias_second)
    return second.astype(jnp.bfloat16).reshape(N_DOM * NODE_DEV, D)
```

```python
import functools

import jax
import jax.numpy as jnp
from jax import lax
from jax.experimental import pallas as pl
from jax.experimental.pallas import tpu as pltpu
from jax.sharding import PartitionSpec as P

WIN = 16
VMEM_LIMIT = 60 * 1024 * 1024


def compose_weights(coef, bases):
    mixed = jnp.einsum(
        "rb,bij->rij", coef, bases.astype(jnp.float32), precision=lax.Precision.HIGHEST
    )
    return mixed.astype(jnp.bfloat16)


def layer_weights(bases, self_weight, coef):
    local_mixed = compose_weights(coef, bases)
    stacked = jnp.concatenate([local_mixed, self_weight[None]], axis=0)
    return lax.all_gather(stacked, "dom", axis=1, tiled=True)


def spread_rows(rows_ref, table_ref, base, parts):
    rows = rows_ref.shape[0]
    step = 256

    def body(chunk, carry):
        first = pl.multiple_of(chunk * step, step)
        for part in range(parts):
            values = rows_ref[pl.ds(first, step), part * 128 : (part + 1) * 128]
            table_ref[pl.ds((base + first) * parts + part, step, stride=parts), :] = values.astype(
                jnp.float32
            )
        return carry

    lax.fori_loop(0, rows // step, body, 0)


def pick_rows(list_ref, major, minor, count, table_ref, held_ref, parts):
    for row in range(count):
        source = list_ref[major, minor + row]
        held_ref[pl.ds(row * parts, parts), :] = table_ref[
            pl.ds(pl.multiple_of(source * parts, parts), parts), :
        ]


def held_rows(held_ref, count, parts):
    return jnp.concatenate(
        [
            held_ref[pl.ds(part, count, stride=parts), :].astype(jnp.bfloat16)
            for part in range(parts)
        ],
        axis=1,
    )


def send_rows_out(send_ref, table_ref, held_a, held_b, out_ref, parts):
    peers, slots = send_ref.shape

    def body(pair, carry):
        for side, held in ((0, held_a), (1, held_b)):
            peer = pair * 2 + side
            pick_rows(send_ref, peer, 0, slots, table_ref, held, parts)
            out_ref[pl.ds(pl.multiple_of(peer * slots, slots), slots), :] = held_rows(
                held, slots, parts
            )
        return carry

    lax.fori_loop(0, peers // 2, body, 0)


def outgoing_kernel(send_ref, rows_ref, out_ref, table_ref, held_a, held_b):
    parts = rows_ref.shape[1] // 128
    spread_rows(rows_ref, table_ref, 0, parts)
    send_rows_out(send_ref, table_ref, held_a, held_b, out_ref, parts)


def layer_kernel(
    last,
    source_ref,
    window_ref,
    count_ref,
    *refs,
):
    if last:
        send_ref = None
        (slot_ref, own_ref, come_ref, weight_ref, bias_ref, out_ref) = refs[:6]
        table_ref, held_a, held_b, pooled_ref, degree_ref = refs[6:]
    else:
        (send_ref, slot_ref, own_ref, come_ref, weight_ref, bias_ref, out_ref, sent_ref) = refs[:8]
        table_ref, held_a, held_b, pooled_ref, degree_ref = refs[8:]
    node_rows, width = own_ref.shape
    parts = width // 128
    tiles, slots, _ = pooled_ref.shape
    relations = slots // WIN
    blocks, block_width = slot_ref.shape
    count = count_ref[0]

    spread_rows(own_ref, table_ref, 0, parts)
    spread_rows(come_ref, table_ref, node_rows, parts)

    def clear(tile, carry):
        pooled_ref[tile] = jnp.zeros(pooled_ref.shape[1:], jnp.float32)
        degree_ref[tile] = jnp.zeros(degree_ref.shape[1:], jnp.float32)
        return carry

    lax.fori_loop(0, tiles, clear, 0)

    slot_ids = lax.broadcasted_iota(jnp.int32, (slots, block_width), 0)
    ones = jnp.ones((block_width, 128), jnp.bfloat16)

    def pool(block, held):
        local = slot_ref[pl.ds(block, 1), :]
        local = jnp.where(block < count, local, -1)
        hot = (slot_ids == local).astype(jnp.float32).astype(jnp.bfloat16)
        sums = jnp.dot(
            hot, held_rows(held, block_width, parts), preferred_element_type=jnp.float32
        )
        numbers = jnp.dot(hot, ones, preferred_element_type=jnp.float32)
        window = window_ref[block]
        pooled_ref[window] += sums
        degree_ref[window] += numbers

    def gather(block, held):
        pick_rows(source_ref, block, 0, block_width, table_ref, held, parts)

    pairs = (count + 1) // 2
    gather(0, held_a)

    def body(pair, carry):
        block = pair * 2
        gather(block + 1, held_b)
        pool(block, held_a)
        gather(jnp.minimum(block + 2, blocks - 1), held_a)
        pool(block + 1, held_b)
        return carry

    lax.fori_loop(0, pairs, body, 0)

    group = 256 // WIN
    bias = bias_ref[...]

    def dense(chunk, carry):
        first = pl.multiple_of(chunk * 256, 256)
        tile = chunk * group
        total = (
            jnp.dot(
                own_ref[pl.ds(first, 256), :],
                weight_ref[relations],
                preferred_element_type=jnp.float32,
            )
            + bias
        )
        for relation in range(relations):
            rows = slice(relation * WIN, (relation + 1) * WIN)
            inverse = 1.0 / jnp.maximum(
                degree_ref[pl.ds(tile, group), rows, :].reshape(256, 128), 1.0
            )
            sums = pooled_ref[pl.ds(tile, group), rows, :].reshape(256, width)
            mean = jnp.concatenate(
                [
                    (sums[:, part * 128 : (part + 1) * 128] * inverse).astype(jnp.bfloat16)
                    for part in range(parts)
                ],
                axis=1,
            )
            total = total + jnp.dot(mean, weight_ref[relation], preferred_element_type=jnp.float32)
        if not last:
            total = jnp.maximum(total, 0.0)
        rounded = total.astype(jnp.bfloat16)
        out_ref[pl.ds(first, 256), :] = rounded
        if not last:
            for part in range(parts):
                table_ref[pl.ds(first * parts + part, 256, stride=parts), :] = rounded[
                    :, part * 128 : (part + 1) * 128
                ].astype(jnp.float32)
        return carry

    lax.fori_loop(0, node_rows // 256, dense, 0)
    if not last:
        send_rows_out(send_ref, table_ref, held_a, held_b, sent_ref, parts)


def in_smem():
    return pl.BlockSpec(memory_space=pltpu.SMEM)


def in_vmem():
    return pl.BlockSpec(memory_space=pltpu.VMEM)


def outgoing_rows(send_rows, rows):
    node_rows, width = rows.shape
    parts = width // 128
    peers, slots = send_rows.shape
    return pl.pallas_call(
        outgoing_kernel,
        out_shape=jax.ShapeDtypeStruct((peers * slots, width), rows.dtype),
        in_specs=[in_smem(), in_vmem()],
        out_specs=in_vmem(),
        scratch_shapes=[
            pltpu.VMEM((node_rows * parts, 128), jnp.float32),
            pltpu.VMEM((slots * parts, 128), jnp.float32),
            pltpu.VMEM((slots * parts, 128), jnp.float32),
        ],
        compiler_params=pltpu.CompilerParams(vmem_limit_bytes=16 * 1024 * 1024),
        name="outgoing",
    )(send_rows, rows)


def relational_layer(last, edges, send_rows, rows, incoming, weights, bias):
    sources, windows, count, local_slot = edges
    node_rows, width = rows.shape
    parts = width // 128
    blocks, block_width = local_slot.shape
    relations = weights.shape[0] - 1
    tiles = node_rows // WIN
    slots = WIN * relations
    table_rows = node_rows + incoming.shape[0]
    result = jax.ShapeDtypeStruct((node_rows, width), rows.dtype)
    if last:
        outs, scalars = result, (sources, windows, count)
    else:
        outs = (result, jax.ShapeDtypeStruct(incoming.shape, rows.dtype))
        scalars = (sources, windows, count, send_rows)
    return pl.pallas_call(
        functools.partial(layer_kernel, last),
        out_shape=outs,
        in_specs=[in_smem()] * len(scalars) + [in_vmem()] * 5,
        out_specs=in_vmem() if last else (in_vmem(), in_vmem()),
        scratch_shapes=[
            pltpu.VMEM((table_rows * parts, 128), jnp.float32),
            pltpu.VMEM((block_width * parts, 128), jnp.float32),
            pltpu.VMEM((block_width * parts, 128), jnp.float32),
            pltpu.VMEM((tiles, slots, width), jnp.float32),
            pltpu.VMEM((tiles, slots, 128), jnp.float32),
        ],
        compiler_params=pltpu.CompilerParams(vmem_limit_bytes=VMEM_LIMIT),
        name="second" if last else "first",
    )(*scalars, local_slot, rows, incoming, weights, bias[None])


def exchange(outgoing, peers):
    slots = outgoing.shape[0] // peers
    shaped = outgoing.reshape(peers, slots, outgoing.shape[1])
    incoming = lax.all_to_all(shaped, "dom", split_axis=0, concat_axis=0, tiled=True)
    return incoming.reshape(outgoing.shape)


def shards(
    features,
    edge_source,
    edge_relation,
    edge_target,
    block_count,
    send_list,
    bases_first,
    self_first,
    coef_first,
    bias_first,
    bases_second,
    self_second,
    coef_second,
    bias_second,
):
    targets = edge_target[0]
    windows = targets[:, 0] // WIN
    local_slot = edge_relation[0] * WIN + targets % WIN
    edges = (edge_source[0], windows, block_count, local_slot)
    send_rows = send_list[0]
    peers = send_rows.shape[0]
    incoming = exchange(outgoing_rows(send_rows, features), peers)
    weights_first = layer_weights(bases_first, self_first, coef_first)
    weights_second = layer_weights(bases_second, self_second, coef_second)
    hidden, outgoing = relational_layer(
        False, edges, send_rows, features, incoming, weights_first, bias_first
    )
    incoming = exchange(outgoing, peers)
    return relational_layer(True, edges, send_rows, hidden, incoming, weights_second, bias_second)


def solution(mesh):
    placed = (
        P("dom", None),
        P("dom", None, None),
        P("dom", None, None),
        P("dom", None, None),
        P("dom"),
        P("dom", None, None),
        P(None, "dom", None),
        P("dom", None),
        P(),
        P(),
        P(None, "dom", None),
        P("dom", None),
        P(),
        P(),
    )
    return jax.shard_map(
        shards, mesh=mesh, in_specs=placed, out_specs=P("dom", None), check_vma=False
    )
```

```python
import functools
import math

import jax
import jax.numpy as jnp
from jax import lax
from jax.experimental import pallas as pl
from jax.experimental.pallas import tpu as pltpu
from jax.sharding import PartitionSpec as P

WIN = 16
VMEM_LIMIT = 40 * 1024 * 1024


def compose_weights(coef, bases):
    mixed = jnp.einsum(
        "rb,bij->rij", coef, bases.astype(jnp.float32), precision=lax.Precision.HIGHEST
    )
    return mixed.astype(jnp.bfloat16)


def weight_share(bases, self_weight, coef):
    local_mixed = compose_weights(coef, bases)
    return jnp.concatenate([local_mixed, self_weight[None]], axis=0)[:, None]


def digits_of(devices):
    chips = devices // 2
    side = max(math.isqrt(chips // 4), 1)
    sizes = (side, side, chips // (side * side))
    digits, stride = [], 2
    for size in sizes:
        digits.append((size, stride))
        stride *= size
    return digits


def shift_pairs(devices, radix, stride, hop):
    pairs = []
    for device in range(devices):
        digit = device // stride % radix
        pairs.append((device, device + ((digit + hop) % radix - digit) * stride))
    return pairs


def send_digit(share, devices, radix, stride):
    return [
        lax.ppermute(share, "dom", shift_pairs(devices, radix, stride, hop))
        for hop in range(1, radix)
    ]


def join_digit(share, came, radix, stride, inner=False):
    if radix == 1:
        return share
    digit = lax.axis_index("dom") // stride % radix
    place = 2 if inner else 1
    if radix == 2:
        low = digit == 0
        parts = [jnp.where(low, share, came[0]), jnp.where(low, came[0], share)]
        full = jnp.stack(parts, axis=place)
    else:
        full = jnp.stack([share] * radix, axis=place)
        for hop, piece in enumerate(came, start=1):
            start = [0] * full.ndim
            start[place] = lax.rem(digit + radix - hop, radix)
            full = lax.dynamic_update_slice(full, jnp.expand_dims(piece, place), start)
    return full.reshape(share.shape[0], share.shape[1] * radix, *share.shape[2:])


def gather_digit(share, devices, radix, stride, inner=False):
    return join_digit(share, send_digit(share, devices, radix, stride), radix, stride, inner)


def spread_rows(rows_ref, table_ref, base, parts):
    rows = rows_ref.shape[0]
    step = 256

    def body(chunk, carry):
        first = pl.multiple_of(chunk * step, step)
        for part in range(parts):
            values = rows_ref[pl.ds(first, step), part * 128 : (part + 1) * 128]
            table_ref[pl.ds((base + first) * parts + part, step, stride=parts), :] = values.astype(
                jnp.float32
            )
        return carry

    lax.fori_loop(0, rows // step, body, 0)


def pick_rows(list_ref, major, minor, count, table_ref, held_ref, parts):
    for row in range(count):
        source = list_ref[major, minor + row]
        held_ref[pl.ds(row * parts, parts), :] = table_ref[
            pl.ds(pl.multiple_of(source * parts, parts), parts), :
        ]


def held_rows(held_ref, count, parts):
    return jnp.concatenate(
        [
            held_ref[pl.ds(part, count, stride=parts), :].astype(jnp.bfloat16)
            for part in range(parts)
        ],
        axis=1,
    )


def send_rows_out(send_ref, table_ref, held_a, held_b, out_ref, parts):
    peers, slots = send_ref.shape

    def body(pair, carry):
        for side, held in ((0, held_a), (1, held_b)):
            peer = pair * 2 + side
            pick_rows(send_ref, peer, 0, slots, table_ref, held, parts)
            out_ref[pl.ds(pl.multiple_of(peer * slots, slots), slots), :] = held_rows(
                held, slots, parts
            )
        return carry

    lax.fori_loop(0, peers // 2, body, 0)


def outgoing_kernel(send_ref, rows_ref, out_ref, table_ref, held_a, held_b):
    parts = rows_ref.shape[1] // 128
    spread_rows(rows_ref, table_ref, 0, parts)
    send_rows_out(send_ref, table_ref, held_a, held_b, out_ref, parts)


def pool_kernel(
    source_ref,
    window_ref,
    count_ref,
    slot_ref,
    own_ref,
    come_ref,
    mean_ref,
    table_ref,
    held_a,
    held_b,
    pooled_ref,
    degree_ref,
):
    node_rows, width = own_ref.shape
    parts = width // 128
    tiles, slots, _ = pooled_ref.shape
    relations = slots // WIN
    blocks, block_width = slot_ref.shape
    count = count_ref[0]

    spread_rows(own_ref, table_ref, 0, parts)
    spread_rows(come_ref, table_ref, node_rows, parts)

    def clear(tile, carry):
        pooled_ref[tile] = jnp.zeros(pooled_ref.shape[1:], jnp.float32)
        degree_ref[tile] = jnp.zeros(degree_ref.shape[1:], jnp.float32)
        return carry

    lax.fori_loop(0, tiles, clear, 0)

    slot_ids = lax.broadcasted_iota(jnp.int32, (slots, block_width), 0)
    ones = jnp.ones((block_width, 128), jnp.bfloat16)

    def pool(block, held):
        local = slot_ref[pl.ds(block, 1), :]
        local = jnp.where(block < count, local, -1)
        hot = (slot_ids == local).astype(jnp.float32).astype(jnp.bfloat16)
        sums = jnp.dot(
            hot, held_rows(held, block_width, parts), preferred_element_type=jnp.float32
        )
        numbers = jnp.dot(hot, ones, preferred_element_type=jnp.float32)
        window = window_ref[block]
        pooled_ref[window] += sums
        degree_ref[window] += numbers

    def gather(block, held):
        block = jnp.minimum(block, blocks - 1)
        pick_rows(source_ref, block, 0, block_width, table_ref, held, parts)

    gather(0, held_a)

    def body(pair, carry):
        block = pair * 2
        gather(block + 1, held_b)
        pool(block, held_a)
        gather(block + 2, held_a)
        pool(jnp.minimum(block + 1, blocks - 1), held_b)
        return carry

    lax.fori_loop(0, (count + 1) // 2, body, 0)

    def average(tile, carry):
        first = pl.multiple_of(tile * WIN, WIN)
        for relation in range(relations):
            rows = slice(relation * WIN, (relation + 1) * WIN)
            inverse = 1.0 / jnp.maximum(degree_ref[tile, rows, :], 1.0)
            for part in range(parts):
                lanes = slice(part * 128, (part + 1) * 128)
                mean_ref[relation, pl.ds(first, WIN), lanes] = (
                    pooled_ref[tile, rows, lanes] * inverse
                ).astype(jnp.bfloat16)
        return carry

    lax.fori_loop(0, tiles, average, 0)


def dense_kernel(last, *refs):
    if last:
        own_ref, mean_ref, weight_ref, bias_ref, out_ref = refs
    else:
        send_ref, own_ref, mean_ref, weight_ref, bias_ref, out_ref, sent_ref = refs[:7]
        table_ref, held_a, held_b = refs[7:]
    node_rows, width = own_ref.shape
    parts = width // 128
    relations = mean_ref.shape[0]
    bias = bias_ref[...]

    def dense(chunk, carry):
        rows = pl.ds(pl.multiple_of(chunk * 256, 256), 256)
        total = bias + jnp.dot(
            own_ref[rows, :], weight_ref[relations], preferred_element_type=jnp.float32
        )
        for relation in range(relations):
            total = total + jnp.dot(
                mean_ref[relation, rows, :],
                weight_ref[relation],
                preferred_element_type=jnp.float32,
            )
        if not last:
            total = jnp.maximum(total, 0.0)
        rounded = total.astype(jnp.bfloat16)
        out_ref[rows, :] = rounded
        if not last:
            for part in range(parts):
                table_ref[pl.ds(chunk * 256 * parts + part, 256, stride=parts), :] = rounded[
                    :, part * 128 : (part + 1) * 128
                ].astype(jnp.float32)
        return carry

    lax.fori_loop(0, node_rows // 256, dense, 0)
    if not last:
        send_rows_out(send_ref, table_ref, held_a, held_b, sent_ref, parts)


def exchange_kernel(devices, out_ref, in_ref, send_sems, recv_sems):
    me = lax.axis_index("dom")

    def copy_to(hop):
        peer = lax.rem(me + hop, devices)
        return pltpu.make_async_remote_copy(
            src_ref=out_ref.at[peer],
            dst_ref=in_ref.at[me],
            send_sem=send_sems.at[hop],
            recv_sem=recv_sems.at[hop],
            device_id=(peer,),
            device_id_type=pl.DeviceIdType.MESH,
        )

    def copy_from(hop):
        peer = lax.rem(me + devices - hop, devices)
        return pltpu.make_async_remote_copy(
            src_ref=out_ref.at[peer],
            dst_ref=in_ref.at[peer],
            send_sem=send_sems.at[hop],
            recv_sem=recv_sems.at[hop],
            device_id=(peer,),
            device_id_type=pl.DeviceIdType.MESH,
        )

    def start(hop, carry):
        copy_to(hop).start()
        return carry

    def finish(hop, carry):
        copy_to(hop).wait_send()
        copy_from(hop).wait_recv()
        return carry

    lax.fori_loop(1, devices, start, 0)
    in_ref[me] = out_ref[me]
    lax.fori_loop(1, devices, finish, 0)


def in_smem():
    return pl.BlockSpec(memory_space=pltpu.SMEM)


def in_vmem():
    return pl.BlockSpec(memory_space=pltpu.VMEM)


def outgoing_rows(send_rows, rows):
    node_rows, width = rows.shape
    parts = width // 128
    peers, slots = send_rows.shape
    return pl.pallas_call(
        outgoing_kernel,
        out_shape=jax.ShapeDtypeStruct((peers * slots, width), rows.dtype),
        in_specs=[in_smem(), in_vmem()],
        out_specs=in_vmem(),
        scratch_shapes=[
            pltpu.VMEM((node_rows * parts, 128), jnp.float32),
            pltpu.VMEM((slots * parts, 128), jnp.float32),
            pltpu.VMEM((slots * parts, 128), jnp.float32),
        ],
        compiler_params=pltpu.CompilerParams(vmem_limit_bytes=16 * 1024 * 1024),
        name="outgoing",
    )(send_rows, rows)


def pooled_means(name, edges, rows, incoming, relations):
    sources, windows, count, local_slot = edges
    node_rows, width = rows.shape
    parts = width // 128
    block_width = local_slot.shape[1]
    tiles = node_rows // WIN
    slots = WIN * relations
    table_rows = node_rows + incoming.shape[0]
    return pl.pallas_call(
        pool_kernel,
        out_shape=jax.ShapeDtypeStruct((relations, node_rows, width), jnp.bfloat16),
        in_specs=[in_smem()] * 3 + [in_vmem()] * 3,
        out_specs=in_vmem(),
        scratch_shapes=[
            pltpu.VMEM((table_rows * parts, 128), jnp.float32),
            pltpu.VMEM((block_width * parts, 128), jnp.float32),
            pltpu.VMEM((block_width * parts, 128), jnp.float32),
            pltpu.VMEM((tiles, slots, width), jnp.float32),
            pltpu.VMEM((tiles, slots, 128), jnp.float32),
        ],
        compiler_params=pltpu.CompilerParams(vmem_limit_bytes=VMEM_LIMIT),
        cost_estimate=pl.CostEstimate(
            flops=20_000_000_000, bytes_accessed=4_000_000, transcendentals=0
        ),
        name=name,
    )(sources, windows, count, local_slot, rows, incoming)


def dense_rows(name, send_rows, rows, means, weights, bias):
    node_rows, width = rows.shape
    parts = width // 128
    last = send_rows is None
    result = jax.ShapeDtypeStruct((node_rows, width), rows.dtype)
    scratch = []
    if not last:
        peers, slots = send_rows.shape
        scratch = [
            pltpu.VMEM((node_rows * parts, 128), jnp.float32),
            pltpu.VMEM((slots * parts, 128), jnp.float32),
            pltpu.VMEM((slots * parts, 128), jnp.float32),
        ]
    return pl.pallas_call(
        functools.partial(dense_kernel, last),
        out_shape=result
        if last
        else (result, jax.ShapeDtypeStruct((peers * slots, width), rows.dtype)),
        in_specs=[in_smem()] * (not last) + [in_vmem()] * 4,
        out_specs=in_vmem() if last else (in_vmem(), in_vmem()),
        scratch_shapes=scratch,
        compiler_params=pltpu.CompilerParams(vmem_limit_bytes=24 * 1024 * 1024),
        cost_estimate=pl.CostEstimate(
            flops=3_000_000_000, bytes_accessed=6_000_000, transcendentals=0
        ),
        name=name,
    )(*([] if last else [send_rows]), rows, means, weights, bias[None])


def exchange(outgoing, peers):
    slots = outgoing.shape[0] // peers
    shaped = outgoing.reshape(peers, slots, outgoing.shape[1])
    incoming = pl.pallas_call(
        functools.partial(exchange_kernel, peers),
        out_shape=jax.ShapeDtypeStruct(shaped.shape, shaped.dtype),
        in_specs=[in_vmem()],
        out_specs=in_vmem(),
        scratch_shapes=[
            pltpu.SemaphoreType.DMA((peers,)),
            pltpu.SemaphoreType.DMA((peers,)),
        ],
        compiler_params=pltpu.CompilerParams(
            has_side_effects=True, vmem_limit_bytes=16 * 1024 * 1024
        ),
        cost_estimate=pl.CostEstimate(
            flops=10_000_000_000, bytes_accessed=1_000_000, transcendentals=0
        ),
        name="exchange",
    )(shaped)
    return incoming.reshape(outgoing.shape)


def shards(
    features,
    edge_source,
    edge_relation,
    edge_target,
    block_count,
    send_list,
    bases_first,
    self_first,
    coef_first,
    bias_first,
    bases_second,
    self_second,
    coef_second,
    bias_second,
):
    targets = edge_target[0]
    windows = targets[:, 0] // WIN
    local_slot = edge_relation[0] * WIN + targets % WIN
    edges = (edge_source[0], windows, block_count, local_slot)
    send_rows = send_list[0]
    peers = send_rows.shape[0]
    relations = coef_first.shape[0]
    width = features.shape[1]
    digits = digits_of(peers)
    share_first = weight_share(bases_first, self_first, coef_first)
    share_second = weight_share(bases_second, self_second, coef_second)

    along_x, along_y, along_z = digits

    early = jnp.concatenate([share_first, share_second], axis=0)
    early = gather_digit(early, peers, *along_x)
    share_first, share_second = early[: relations + 1], early[relations + 1 :]
    share_first = gather_digit(share_first, peers, *along_y)
    outgoing = outgoing_rows(send_rows, features)
    outgoing, share_first, share_second = lax.optimization_barrier(
        (outgoing, share_first, share_second)
    )
    incoming = exchange(outgoing, peers)
    incoming, share_first, share_second = lax.optimization_barrier(
        (incoming, share_first, share_second)
    )
    came_second = send_digit(share_second, peers, *along_y)
    came_first = send_digit(share_first, peers, *along_z)
    means = pooled_means("pool_first", edges, features, incoming, relations)
    means, came_first, came_second = lax.optimization_barrier((means, came_first, came_second))
    share_first = gather_digit(join_digit(share_first, came_first, *along_z), peers, 2, 1, True)
    share_second = join_digit(share_second, came_second, *along_y)
    weights_first = share_first.reshape(relations + 1, width, width)
    hidden, outgoing = dense_rows(
        "dense_first", send_rows, features, means, weights_first, bias_first
    )
    incoming = exchange(outgoing, peers)
    incoming, share_second = lax.optimization_barrier((incoming, share_second))
    came_second = send_digit(share_second, peers, *along_z)
    means = pooled_means("pool_second", edges, hidden, incoming, relations)
    means, came_second = lax.optimization_barrier((means, came_second))
    share_second = gather_digit(
        join_digit(share_second, came_second, *along_z), peers, 2, 1, True
    )
    weights_second = share_second.reshape(relations + 1, width, width)
    return dense_rows("dense_second", None, hidden, means, weights_second, bias_second)


def solution(mesh):
    placed = (
        P("dom", None),
        P("dom", None, None),
        P("dom", None, None),
        P("dom", None, None),
        P("dom"),
        P("dom", None, None),
        P(None, "dom", None),
        P("dom", None),
        P(),
        P(),
        P(None, "dom", None),
        P("dom", None),
        P(),
        P(),
    )
    return jax.shard_map(
        shards, mesh=mesh, in_specs=placed, out_specs=P("dom", None), check_vma=False
    )
```

```python
import functools
import math

import jax
import jax.numpy as jnp
from jax import lax
from jax.experimental import pallas as pl
from jax.experimental.pallas import tpu as pltpu
from jax.sharding import PartitionSpec as P

WIN = 16
VMEM_LIMIT = 40 * 1024 * 1024


def compose_weights(coef, bases):
    mixed = jnp.einsum(
        "rb,bij->rij", coef, bases.astype(jnp.float32), precision=lax.Precision.HIGHEST
    )
    return mixed.astype(jnp.bfloat16)


def weight_share(bases, self_weight, coef):
    local_mixed = compose_weights(coef, bases)
    return jnp.concatenate([local_mixed, self_weight[None]], axis=0)[:, None]


def digits_of(devices):
    chips = devices // 2
    side = max(math.isqrt(chips // 4), 1)
    sizes = (side, side, chips // (side * side))
    digits, stride = [], 2
    for size in sizes:
        digits.append((size, stride))
        stride *= size
    return digits


def shift_pairs(devices, radix, stride, hop):
    pairs = []
    for device in range(devices):
        digit = device // stride % radix
        pairs.append((device, device + ((digit + hop) % radix - digit) * stride))
    return pairs


def send_digit(share, devices, radix, stride):
    return [
        lax.ppermute(share, "dom", shift_pairs(devices, radix, stride, hop))
        for hop in range(1, radix)
    ]


def join_digit(share, came, radix, stride, inner=False):
    if radix == 1:
        return share
    digit = lax.axis_index("dom") // stride % radix
    place = 2 if inner else 1
    if radix == 2:
        low = digit == 0
        parts = [jnp.where(low, share, came[0]), jnp.where(low, came[0], share)]
        full = jnp.stack(parts, axis=place)
    else:
        full = jnp.stack([share] * radix, axis=place)
        for hop, piece in enumerate(came, start=1):
            start = [0] * full.ndim
            start[place] = lax.rem(digit + radix - hop, radix)
            full = lax.dynamic_update_slice(full, jnp.expand_dims(piece, place), start)
    return full.reshape(share.shape[0], share.shape[1] * radix, *share.shape[2:])


def gather_digit(share, devices, radix, stride, inner=False):
    return join_digit(share, send_digit(share, devices, radix, stride), radix, stride, inner)


def spread_rows(rows_ref, table_ref, base, parts):
    rows = rows_ref.shape[0]
    step = 256

    def body(chunk, carry):
        first = pl.multiple_of(chunk * step, step)
        for part in range(parts):
            values = rows_ref[pl.ds(first, step), part * 128 : (part + 1) * 128]
            table_ref[pl.ds((base + first) * parts + part, step, stride=parts), :] = values.astype(
                jnp.float32
            )
        return carry

    lax.fori_loop(0, rows // step, body, 0)


def pick_rows(list_ref, major, minor, count, table_ref, held_ref, parts):
    listed = list_ref.at[major]
    for row in range(count):
        source = listed[minor + row]
        held_ref[pl.ds(row * parts, parts), :] = table_ref[
            pl.ds(pl.multiple_of(source, parts), parts), :
        ]


def held_rows(held_ref, count, parts):
    return jnp.concatenate(
        [
            held_ref[pl.ds(part, count, stride=parts), :].astype(jnp.bfloat16)
            for part in range(parts)
        ],
        axis=1,
    )


def send_rows_out(send_ref, table_ref, held_a, held_b, out_ref, parts):
    peers, slots = send_ref.shape

    def body(pair, carry):
        for side, held in ((0, held_a), (1, held_b)):
            peer = pair * 2 + side
            pick_rows(send_ref, peer, 0, slots, table_ref, held, parts)
            out_ref[pl.ds(pl.multiple_of(peer * slots, slots), slots), :] = held_rows(
                held, slots, parts
            )
        return carry

    lax.fori_loop(0, peers // 2, body, 0)


def outgoing_kernel(send_ref, rows_ref, out_ref, table_ref, held_a, held_b):
    parts = rows_ref.shape[1] // 128
    spread_rows(rows_ref, table_ref, 0, parts)
    send_rows_out(send_ref, table_ref, held_a, held_b, out_ref, parts)


def pool_kernel(
    source_ref,
    window_ref,
    count_ref,
    slot_ref,
    own_ref,
    come_ref,
    mean_ref,
    table_ref,
    held_a,
    held_b,
    pooled_ref,
    degree_ref,
):
    node_rows, width = own_ref.shape
    parts = width // 128
    tiles, slots, _ = pooled_ref.shape
    relations = slots // WIN
    blocks, block_width = slot_ref.shape
    count = count_ref[0]

    spread_rows(own_ref, table_ref, 0, parts)
    spread_rows(come_ref, table_ref, node_rows, parts)

    def clear(tile, carry):
        pooled_ref[tile] = jnp.zeros(pooled_ref.shape[1:], jnp.float32)
        degree_ref[tile] = jnp.zeros(degree_ref.shape[1:], jnp.float32)
        return carry

    lax.fori_loop(0, tiles, clear, 0)

    slot_ids = lax.broadcasted_iota(jnp.int32, (slots, block_width), 0)
    ones = jnp.ones((block_width, 128), jnp.bfloat16)

    def pool(block, held):
        local = slot_ref[pl.ds(block, 1), :]
        local = jnp.where(block < count, local, -1)
        hot = (slot_ids == local).astype(jnp.float32).astype(jnp.bfloat16)
        sums = jnp.dot(
            hot, held_rows(held, block_width, parts), preferred_element_type=jnp.float32
        )
        numbers = jnp.dot(hot, ones, preferred_element_type=jnp.float32)
        window = window_ref[block]
        pooled_ref[window] += sums
        degree_ref[window] += numbers

    def gather(block, held):
        block = jnp.minimum(block, blocks - 1)
        pick_rows(source_ref, block, 0, block_width, table_ref, held, parts)

    gather(0, held_a)

    def body(pair, carry):
        block = pair * 2
        gather(block + 1, held_b)
        pool(block, held_a)
        gather(block + 2, held_a)
        pool(jnp.minimum(block + 1, blocks - 1), held_b)
        return carry

    lax.fori_loop(0, (count + 1) // 2, body, 0)

    def average(tile, carry):
        first = pl.multiple_of(tile * WIN, WIN)
        for relation in range(relations):
            rows = slice(relation * WIN, (relation + 1) * WIN)
            inverse = 1.0 / jnp.maximum(degree_ref[tile, rows, :], 1.0)
            for part in range(parts):
                lanes = slice(part * 128, (part + 1) * 128)
                mean_ref[relation, pl.ds(first, WIN), lanes] = (
                    pooled_ref[tile, rows, lanes] * inverse
                ).astype(jnp.bfloat16)
        return carry

    lax.fori_loop(0, tiles, average, 0)


def dense_kernel(last, *refs):
    if last:
        own_ref, mean_ref, weight_ref, bias_ref, out_ref = refs
    else:
        send_ref, own_ref, mean_ref, weight_ref, bias_ref, out_ref, sent_ref = refs[:7]
        table_ref, held_a, held_b = refs[7:]
    node_rows, width = own_ref.shape
    parts = width // 128
    relations = mean_ref.shape[0]
    bias = bias_ref[...]

    def dense(chunk, carry):
        rows = pl.ds(pl.multiple_of(chunk * 256, 256), 256)
        total = bias + jnp.dot(
            own_ref[rows, :], weight_ref[relations], preferred_element_type=jnp.float32
        )
        for relation in range(relations):
            total = total + jnp.dot(
                mean_ref[relation, rows, :],
                weight_ref[relation],
                preferred_element_type=jnp.float32,
            )
        if not last:
            total = jnp.maximum(total, 0.0)
        rounded = total.astype(jnp.bfloat16)
        out_ref[rows, :] = rounded
        if not last:
            for part in range(parts):
                table_ref[pl.ds(chunk * 256 * parts + part, 256, stride=parts), :] = rounded[
                    :, part * 128 : (part + 1) * 128
                ].astype(jnp.float32)
        return carry

    lax.fori_loop(0, node_rows // 256, dense, 0)
    if not last:
        send_rows_out(send_ref, table_ref, held_a, held_b, sent_ref, parts)


def exchange_kernel(devices, out_ref, in_ref, send_sems, recv_sems):
    me = lax.axis_index("dom")

    def copy_to(hop):
        peer = lax.rem(me + hop, devices)
        return pltpu.make_async_remote_copy(
            src_ref=out_ref.at[peer],
            dst_ref=in_ref.at[me],
            send_sem=send_sems.at[hop],
            recv_sem=recv_sems.at[hop],
            device_id=(peer,),
            device_id_type=pl.DeviceIdType.MESH,
        )

    def copy_from(hop):
        peer = lax.rem(me + devices - hop, devices)
        return pltpu.make_async_remote_copy(
            src_ref=out_ref.at[peer],
            dst_ref=in_ref.at[peer],
            send_sem=send_sems.at[hop],
            recv_sem=recv_sems.at[hop],
            device_id=(peer,),
            device_id_type=pl.DeviceIdType.MESH,
        )

    def start(hop, carry):
        copy_to(hop).start()
        return carry

    def finish(hop, carry):
        copy_to(hop).wait_send()
        copy_from(hop).wait_recv()
        return carry

    lax.fori_loop(1, devices, start, 0)
    in_ref[me] = out_ref[me]
    lax.fori_loop(1, devices, finish, 0)


def in_smem():
    return pl.BlockSpec(memory_space=pltpu.SMEM)


def in_vmem():
    return pl.BlockSpec(memory_space=pltpu.VMEM)


def outgoing_rows(send_rows, rows):
    node_rows, width = rows.shape
    parts = width // 128
    peers, slots = send_rows.shape
    return pl.pallas_call(
        outgoing_kernel,
        out_shape=jax.ShapeDtypeStruct((peers * slots, width), rows.dtype),
        in_specs=[in_smem(), in_vmem()],
        out_specs=in_vmem(),
        scratch_shapes=[
            pltpu.VMEM((node_rows * parts, 128), jnp.float32),
            pltpu.VMEM((slots * parts, 128), jnp.float32),
            pltpu.VMEM((slots * parts, 128), jnp.float32),
        ],
        compiler_params=pltpu.CompilerParams(vmem_limit_bytes=16 * 1024 * 1024),
        name="outgoing",
    )(send_rows, rows)


def pooled_means(name, edges, rows, incoming, relations):
    sources, windows, count, local_slot = edges
    node_rows, width = rows.shape
    parts = width // 128
    block_width = local_slot.shape[1]
    tiles = node_rows // WIN
    slots = WIN * relations
    table_rows = node_rows + incoming.shape[0]
    return pl.pallas_call(
        pool_kernel,
        out_shape=jax.ShapeDtypeStruct((relations, node_rows, width), jnp.bfloat16),
        in_specs=[in_smem()] * 3 + [in_vmem()] * 3,
        out_specs=in_vmem(),
        scratch_shapes=[
            pltpu.VMEM((table_rows * parts, 128), jnp.float32),
            pltpu.VMEM((block_width * parts, 128), jnp.float32),
            pltpu.VMEM((block_width * parts, 128), jnp.float32),
            pltpu.VMEM((tiles, slots, width), jnp.float32),
            pltpu.VMEM((tiles, slots, 128), jnp.float32),
        ],
        compiler_params=pltpu.CompilerParams(vmem_limit_bytes=VMEM_LIMIT),
        cost_estimate=pl.CostEstimate(
            flops=20_000_000_000, bytes_accessed=4_000_000, transcendentals=0
        ),
        name=name,
    )(sources, windows, count, local_slot, rows, incoming)


def dense_rows(name, send_rows, rows, means, weights, bias):
    node_rows, width = rows.shape
    parts = width // 128
    last = send_rows is None
    result = jax.ShapeDtypeStruct((node_rows, width), rows.dtype)
    scratch = []
    if not last:
        peers, slots = send_rows.shape
        scratch = [
            pltpu.VMEM((node_rows * parts, 128), jnp.float32),
            pltpu.VMEM((slots * parts, 128), jnp.float32),
            pltpu.VMEM((slots * parts, 128), jnp.float32),
        ]
    return pl.pallas_call(
        functools.partial(dense_kernel, last),
        out_shape=result
        if last
        else (result, jax.ShapeDtypeStruct((peers * slots, width), rows.dtype)),
        in_specs=[in_smem()] * (not last) + [in_vmem()] * 4,
        out_specs=in_vmem() if last else (in_vmem(), in_vmem()),
        scratch_shapes=scratch,
        compiler_params=pltpu.CompilerParams(vmem_limit_bytes=24 * 1024 * 1024),
        cost_estimate=pl.CostEstimate(
            flops=3_000_000_000, bytes_accessed=6_000_000, transcendentals=0
        ),
        name=name,
    )(*([] if last else [send_rows]), rows, means, weights, bias[None])


def exchange(outgoing, peers):
    slots = outgoing.shape[0] // peers
    shaped = outgoing.reshape(peers, slots, outgoing.shape[1])
    incoming = pl.pallas_call(
        functools.partial(exchange_kernel, peers),
        out_shape=jax.ShapeDtypeStruct(shaped.shape, shaped.dtype),
        in_specs=[in_vmem()],
        out_specs=in_vmem(),
        scratch_shapes=[
            pltpu.SemaphoreType.DMA((peers,)),
            pltpu.SemaphoreType.DMA((peers,)),
        ],
        compiler_params=pltpu.CompilerParams(
            has_side_effects=True, vmem_limit_bytes=16 * 1024 * 1024
        ),
        cost_estimate=pl.CostEstimate(
            flops=10_000_000_000, bytes_accessed=1_000_000, transcendentals=0
        ),
        name="exchange",
    )(shaped)
    return incoming.reshape(outgoing.shape)


def shards(
    features,
    edge_source,
    edge_relation,
    edge_target,
    block_count,
    send_list,
    bases_first,
    self_first,
    coef_first,
    bias_first,
    bases_second,
    self_second,
    coef_second,
    bias_second,
):
    targets = edge_target[0]
    windows = targets[:, 0] // WIN
    local_slot = edge_relation[0] * WIN + targets % WIN
    lanes = features.shape[1] // 128
    edges = (edge_source[0] * lanes, windows, block_count, local_slot)
    send_rows = send_list[0] * lanes
    peers = send_rows.shape[0]
    relations = coef_first.shape[0]
    width = features.shape[1]
    digits = digits_of(peers)
    share_first = weight_share(bases_first, self_first, coef_first)
    share_second = weight_share(bases_second, self_second, coef_second)

    along_x, along_y, along_z = digits

    early = jnp.concatenate([share_first, share_second], axis=0)
    early = gather_digit(early, peers, *along_x)
    share_first, share_second = early[: relations + 1], early[relations + 1 :]
    share_first = gather_digit(share_first, peers, *along_y)
    outgoing = outgoing_rows(send_rows, features)
    outgoing, share_first, share_second = lax.optimization_barrier(
        (outgoing, share_first, share_second)
    )
    incoming = exchange(outgoing, peers)
    incoming, share_first, share_second = lax.optimization_barrier(
        (incoming, share_first, share_second)
    )
    came_second = send_digit(share_second, peers, *along_y)
    came_first = send_digit(share_first, peers, *along_z)
    means = pooled_means("pool_first", edges, features, incoming, relations)
    means, came_first, came_second = lax.optimization_barrier((means, came_first, came_second))
    share_first = gather_digit(join_digit(share_first, came_first, *along_z), peers, 2, 1, True)
    share_second = join_digit(share_second, came_second, *along_y)
    weights_first = share_first.reshape(relations + 1, width, width)
    hidden, outgoing = dense_rows(
        "dense_first", send_rows, features, means, weights_first, bias_first
    )
    incoming = exchange(outgoing, peers)
    incoming, share_second = lax.optimization_barrier((incoming, share_second))
    came_second = send_digit(share_second, peers, *along_z)
    means = pooled_means("pool_second", edges, hidden, incoming, relations)
    means, came_second = lax.optimization_barrier((means, came_second))
    share_second = gather_digit(
        join_digit(share_second, came_second, *along_z), peers, 2, 1, True
    )
    weights_second = share_second.reshape(relations + 1, width, width)
    return dense_rows("dense_second", None, hidden, means, weights_second, bias_second)


def solution(mesh):
    placed = (
        P("dom", None),
        P("dom", None, None),
        P("dom", None, None),
        P("dom", None, None),
        P("dom"),
        P("dom", None, None),
        P(None, "dom", None),
        P("dom", None),
        P(),
        P(),
        P(None, "dom", None),
        P("dom", None),
        P(),
        P(),
    )
    return jax.shard_map(
        shards, mesh=mesh, in_specs=placed, out_specs=P("dom", None), check_vma=False
    )
```

```python
import functools
import math

import jax
import jax.numpy as jnp
from jax import lax
from jax.experimental import pallas as pl
from jax.experimental.pallas import tpu as pltpu
from jax.sharding import PartitionSpec as P

WIN = 16
VMEM_LIMIT = 40 * 1024 * 1024


def compose_weights(coef, bases):
    mixed = jnp.einsum(
        "rb,bij->rij", coef, bases.astype(jnp.float32), precision=lax.Precision.HIGHEST
    )
    return mixed.astype(jnp.bfloat16)


def weight_share(bases, self_weight, coef):
    local_mixed = compose_weights(coef, bases)
    return jnp.concatenate([local_mixed, self_weight[None]], axis=0)[:, None]


def digits_of(devices):
    chips = devices // 2
    side = max(math.isqrt(chips // 4), 1)
    sizes = (side, side, chips // (side * side))
    digits, stride = [], 2
    for size in sizes:
        digits.append((size, stride))
        stride *= size
    return digits


def shift_pairs(devices, radix, stride, hop):
    pairs = []
    for device in range(devices):
        digit = device // stride % radix
        pairs.append((device, device + ((digit + hop) % radix - digit) * stride))
    return pairs


def send_digit(share, devices, radix, stride):
    return [
        lax.ppermute(share, "dom", shift_pairs(devices, radix, stride, hop))
        for hop in range(1, radix)
    ]


def join_digit(share, came, radix, stride, inner=False):
    if radix == 1:
        return share
    digit = lax.axis_index("dom") // stride % radix
    place = 2 if inner else 1
    if radix == 2:
        low = digit == 0
        parts = [jnp.where(low, share, came[0]), jnp.where(low, came[0], share)]
        full = jnp.stack(parts, axis=place)
    else:
        full = jnp.stack([share] * radix, axis=place)
        for hop, piece in enumerate(came, start=1):
            start = [0] * full.ndim
            start[place] = lax.rem(digit + radix - hop, radix)
            full = lax.dynamic_update_slice(full, jnp.expand_dims(piece, place), start)
    return full.reshape(share.shape[0], share.shape[1] * radix, *share.shape[2:])


def gather_digit(share, devices, radix, stride, inner=False):
    return join_digit(share, send_digit(share, devices, radix, stride), radix, stride, inner)


def spread_rows(rows_ref, table_ref, base, parts):
    rows = rows_ref.shape[0]
    step = 256

    def body(chunk, carry):
        first = pl.multiple_of(chunk * step, step)
        for part in range(parts):
            values = rows_ref[pl.ds(first, step), part * 128 : (part + 1) * 128]
            table_ref[pl.ds((base + first) * parts + part, step, stride=parts), :] = values.astype(
                jnp.float32
            )
        return carry

    lax.fori_loop(0, rows // step, body, 0)


def pick_rows(list_ref, major, minor, count, table_ref, held_ref, parts):
    listed = list_ref.at[major]
    for row in range(count):
        source = listed[minor + row]
        held_ref[pl.ds(row * parts, parts), :] = table_ref[
            pl.ds(pl.multiple_of(source, parts), parts), :
        ]


def held_rows(held_ref, count, parts):
    return jnp.concatenate(
        [
            held_ref[pl.ds(part, count, stride=parts), :].astype(jnp.bfloat16)
            for part in range(parts)
        ],
        axis=1,
    )


def send_rows_out(send_ref, table_ref, held_a, held_b, out_ref, parts):
    peers, slots = send_ref.shape

    def body(pair, carry):
        for side, held in ((0, held_a), (1, held_b)):
            peer = pair * 2 + side
            pick_rows(send_ref, peer, 0, slots, table_ref, held, parts)
            out_ref[pl.ds(pl.multiple_of(peer * slots, slots), slots), :] = held_rows(
                held, slots, parts
            )
        return carry

    lax.fori_loop(0, peers // 2, body, 0)


def outgoing_kernel(send_ref, rows_ref, out_ref, table_ref, held_a, held_b):
    parts = rows_ref.shape[1] // 128
    spread_rows(rows_ref, table_ref, 0, parts)
    send_rows_out(send_ref, table_ref, held_a, held_b, out_ref, parts)


def pool_kernel(
    source_ref,
    window_ref,
    count_ref,
    slot_ref,
    own_ref,
    come_ref,
    mean_ref,
    table_ref,
    held_a,
    held_b,
    pooled_ref,
    degree_ref,
):
    node_rows, width = own_ref.shape
    parts = width // 128
    tiles, slots, _ = pooled_ref.shape
    relations = slots // WIN
    blocks, block_width = slot_ref.shape
    count = count_ref[0]

    spread_rows(own_ref, table_ref, 0, parts)
    spread_rows(come_ref, table_ref, node_rows, parts)

    def clear(tile, carry):
        pooled_ref[tile] = jnp.zeros(pooled_ref.shape[1:], jnp.float32)
        degree_ref[tile] = jnp.zeros(degree_ref.shape[1:], jnp.float32)
        return carry

    lax.fori_loop(0, tiles, clear, 0)

    slot_ids = lax.broadcasted_iota(jnp.int32, (slots, block_width), 0)
    ones = jnp.ones((block_width, 128), jnp.bfloat16)

    def pool(block, held):
        local = slot_ref[pl.ds(block, 1), :]
        local = jnp.where(block < count, local, -1)
        hot = (slot_ids == local).astype(jnp.float32).astype(jnp.bfloat16)
        sums = jnp.dot(
            hot, held_rows(held, block_width, parts), preferred_element_type=jnp.float32
        )
        numbers = jnp.dot(hot, ones, preferred_element_type=jnp.float32)
        window = window_ref[block]
        pooled_ref[window] += sums
        degree_ref[window] += numbers

    def gather(block, held):
        block = jnp.minimum(block, blocks - 1)
        pick_rows(source_ref, block, 0, block_width, table_ref, held, parts)

    gather(0, held_a)

    def body(pair, carry):
        block = pair * 2
        gather(block + 1, held_b)
        pool(block, held_a)
        gather(block + 2, held_a)
        pool(jnp.minimum(block + 1, blocks - 1), held_b)
        return carry

    lax.fori_loop(0, (count + 1) // 2, body, 0)

    def average(tile, carry):
        first = pl.multiple_of(tile * WIN, WIN)
        for relation in range(relations):
            rows = slice(relation * WIN, (relation + 1) * WIN)
            inverse = 1.0 / jnp.maximum(degree_ref[tile, rows, :], 1.0)
            for part in range(parts):
                lanes = slice(part * 128, (part + 1) * 128)
                mean_ref[relation, pl.ds(first, WIN), lanes] = (
                    pooled_ref[tile, rows, lanes] * inverse
                ).astype(jnp.bfloat16)
        return carry

    lax.fori_loop(0, tiles, average, 0)


def dense_kernel(last, *refs):
    if last:
        own_ref, mean_ref, weight_ref, bias_ref, out_ref = refs
    else:
        send_ref, own_ref, mean_ref, weight_ref, bias_ref, out_ref, sent_ref = refs[:7]
        table_ref, held_a, held_b = refs[7:]
    node_rows, width = own_ref.shape
    parts = width // 128
    relations = mean_ref.shape[0]
    bias = bias_ref[...]

    def dense(chunk, carry):
        rows = pl.ds(pl.multiple_of(chunk * 256, 256), 256)
        total = bias + jnp.dot(
            own_ref[rows, :], weight_ref[relations], preferred_element_type=jnp.float32
        )
        for relation in range(relations):
            total = total + jnp.dot(
                mean_ref[relation, rows, :],
                weight_ref[relation],
                preferred_element_type=jnp.float32,
            )
        if not last:
            total = jnp.maximum(total, 0.0)
        rounded = total.astype(jnp.bfloat16)
        out_ref[rows, :] = rounded
        if not last:
            for part in range(parts):
                table_ref[pl.ds(chunk * 256 * parts + part, 256, stride=parts), :] = rounded[
                    :, part * 128 : (part + 1) * 128
                ].astype(jnp.float32)
        return carry

    lax.fori_loop(0, node_rows // 256, dense, 0)
    if not last:
        send_rows_out(send_ref, table_ref, held_a, held_b, sent_ref, parts)


def exchange_kernel(devices, out_ref, in_ref, send_sems, recv_sems):
    me = lax.axis_index("dom")

    def copy_to(hop):
        peer = lax.rem(me + hop, devices)
        return pltpu.make_async_remote_copy(
            src_ref=out_ref.at[peer],
            dst_ref=in_ref.at[me],
            send_sem=send_sems.at[hop],
            recv_sem=recv_sems.at[hop],
            device_id=(peer,),
            device_id_type=pl.DeviceIdType.MESH,
        )

    def copy_from(hop):
        peer = lax.rem(me + devices - hop, devices)
        return pltpu.make_async_remote_copy(
            src_ref=out_ref.at[peer],
            dst_ref=in_ref.at[peer],
            send_sem=send_sems.at[hop],
            recv_sem=recv_sems.at[hop],
            device_id=(peer,),
            device_id_type=pl.DeviceIdType.MESH,
        )

    def start(hop, carry):
        copy_to(hop).start()
        return carry

    def finish(hop, carry):
        copy_to(hop).wait_send()
        copy_from(hop).wait_recv()
        return carry

    lax.fori_loop(1, devices, start, 0)
    in_ref[me] = out_ref[me]
    lax.fori_loop(1, devices, finish, 0)


def in_smem():
    return pl.BlockSpec(memory_space=pltpu.SMEM)


def in_vmem():
    return pl.BlockSpec(memory_space=pltpu.VMEM)


def outgoing_rows(send_rows, rows):
    node_rows, width = rows.shape
    parts = width // 128
    peers, slots = send_rows.shape
    return pl.pallas_call(
        outgoing_kernel,
        out_shape=jax.ShapeDtypeStruct((peers * slots, width), rows.dtype),
        in_specs=[in_smem(), in_vmem()],
        out_specs=in_vmem(),
        scratch_shapes=[
            pltpu.VMEM((node_rows * parts, 128), jnp.float32),
            pltpu.VMEM((slots * parts, 128), jnp.float32),
            pltpu.VMEM((slots * parts, 128), jnp.float32),
        ],
        compiler_params=pltpu.CompilerParams(vmem_limit_bytes=16 * 1024 * 1024),
        name="outgoing",
    )(send_rows, rows)


def pooled_means(name, edges, rows, incoming, relations):
    sources, windows, count, local_slot = edges
    node_rows, width = rows.shape
    parts = width // 128
    block_width = local_slot.shape[1]
    tiles = node_rows // WIN
    slots = WIN * relations
    table_rows = node_rows + incoming.shape[0]
    return pl.pallas_call(
        pool_kernel,
        out_shape=jax.ShapeDtypeStruct((relations, node_rows, width), jnp.bfloat16),
        in_specs=[in_smem()] * 3 + [in_vmem()] * 3,
        out_specs=in_vmem(),
        scratch_shapes=[
            pltpu.VMEM((table_rows * parts, 128), jnp.float32),
            pltpu.VMEM((block_width * parts, 128), jnp.float32),
            pltpu.VMEM((block_width * parts, 128), jnp.float32),
            pltpu.VMEM((tiles, slots, width), jnp.float32),
            pltpu.VMEM((tiles, slots, 128), jnp.float32),
        ],
        compiler_params=pltpu.CompilerParams(vmem_limit_bytes=VMEM_LIMIT),
        cost_estimate=pl.CostEstimate(
            flops=20_000_000_000, bytes_accessed=4_000_000, transcendentals=0
        ),
        name=name,
    )(sources, windows, count, local_slot, rows, incoming)


def dense_rows(name, send_rows, rows, means, weights, bias):
    node_rows, width = rows.shape
    parts = width // 128
    last = send_rows is None
    result = jax.ShapeDtypeStruct((node_rows, width), rows.dtype)
    scratch = []
    if not last:
        peers, slots = send_rows.shape
        scratch = [
            pltpu.VMEM((node_rows * parts, 128), jnp.float32),
            pltpu.VMEM((slots * parts, 128), jnp.float32),
            pltpu.VMEM((slots * parts, 128), jnp.float32),
        ]
    return pl.pallas_call(
        functools.partial(dense_kernel, last),
        out_shape=result
        if last
        else (result, jax.ShapeDtypeStruct((peers * slots, width), rows.dtype)),
        in_specs=[in_smem()] * (not last) + [in_vmem()] * 4,
        out_specs=in_vmem() if last else (in_vmem(), in_vmem()),
        scratch_shapes=scratch,
        compiler_params=pltpu.CompilerParams(vmem_limit_bytes=24 * 1024 * 1024),
        cost_estimate=pl.CostEstimate(
            flops=3_000_000_000, bytes_accessed=6_000_000, transcendentals=0
        ),
        name=name,
    )(*([] if last else [send_rows]), rows, means, weights, bias[None])


def exchange(outgoing, peers):
    slots = outgoing.shape[0] // peers
    shaped = outgoing.reshape(peers, slots, outgoing.shape[1])
    incoming = pl.pallas_call(
        functools.partial(exchange_kernel, peers),
        out_shape=jax.ShapeDtypeStruct(shaped.shape, shaped.dtype),
        in_specs=[in_vmem()],
        out_specs=in_vmem(),
        scratch_shapes=[
            pltpu.SemaphoreType.DMA((peers,)),
            pltpu.SemaphoreType.DMA((peers,)),
        ],
        compiler_params=pltpu.CompilerParams(
            has_side_effects=True, vmem_limit_bytes=16 * 1024 * 1024
        ),
        cost_estimate=pl.CostEstimate(
            flops=10_000_000_000, bytes_accessed=1_000_000, transcendentals=0
        ),
        name="exchange",
    )(shaped)
    return incoming.reshape(outgoing.shape)


def shards(
    features,
    edge_source,
    edge_relation,
    edge_target,
    block_count,
    send_list,
    bases_first,
    self_first,
    coef_first,
    bias_first,
    bases_second,
    self_second,
    coef_second,
    bias_second,
):
    targets = edge_target[0]
    windows = targets[:, 0] // WIN
    local_slot = edge_relation[0] * WIN + targets % WIN
    lanes = features.shape[1] // 128
    edges = (edge_source[0] * lanes, windows, block_count, local_slot)
    send_rows = send_list[0] * lanes
    peers = send_rows.shape[0]
    relations = coef_first.shape[0]
    width = features.shape[1]
    digits = digits_of(peers)
    share_first = weight_share(bases_first, self_first, coef_first)
    share_second = weight_share(bases_second, self_second, coef_second)

    along_x, along_y, along_z = digits

    early = jnp.concatenate([share_first, share_second], axis=0)
    early = gather_digit(early, peers, *along_x)
    share_first, share_second = early[: relations + 1], early[relations + 1 :]
    came_first = send_digit(share_first, peers, *along_y)
    incoming = exchange(outgoing_rows(send_rows, features), peers)
    incoming, came_first, share_first, share_second = lax.optimization_barrier(
        (incoming, came_first, share_first, share_second)
    )
    share_first = join_digit(share_first, came_first, *along_y)
    came_second = send_digit(share_second, peers, *along_y)
    came_first = send_digit(share_first, peers, *along_z)
    means = pooled_means("pool_first", edges, features, incoming, relations)
    means, came_first, came_second = lax.optimization_barrier((means, came_first, came_second))
    share_first = gather_digit(join_digit(share_first, came_first, *along_z), peers, 2, 1, True)
    share_second = join_digit(share_second, came_second, *along_y)
    weights_first = share_first.reshape(relations + 1, width, width)
    hidden, outgoing = dense_rows(
        "dense_first", send_rows, features, means, weights_first, bias_first
    )
    incoming = exchange(outgoing, peers)
    incoming, share_second = lax.optimization_barrier((incoming, share_second))
    came_second = send_digit(share_second, peers, *along_z)
    means = pooled_means("pool_second", edges, hidden, incoming, relations)
    means, came_second = lax.optimization_barrier((means, came_second))
    share_second = gather_digit(
        join_digit(share_second, came_second, *along_z), peers, 2, 1, True
    )
    weights_second = share_second.reshape(relations + 1, width, width)
    return dense_rows("dense_second", None, hidden, means, weights_second, bias_second)


def solution(mesh):
    placed = (
        P("dom", None),
        P("dom", None, None),
        P("dom", None, None),
        P("dom", None, None),
        P("dom"),
        P("dom", None, None),
        P(None, "dom", None),
        P("dom", None),
        P(),
        P(),
        P(None, "dom", None),
        P("dom", None),
        P(),
        P(),
    )
    return jax.shard_map(
        shards, mesh=mesh, in_specs=placed, out_specs=P("dom", None), check_vma=False
    )
```
